256 devices in a mesh: row: 16 (over z, x_lo), col: 16 (over x_hi, y, core).
Axes of the slice: x: 4 (x_hi: 2, x_lo: 2; x = x_hi * 2 + x_lo), y: 4, z: 8, core: 2. Of those that a mesh axis runs over, the one named last changes fastest.
Arguments:
- field: bfloat16 [128, 2048, 2048], P(None, 'row', 'col'), may hold values from -6 to 6
- solid_flags: int32 [128, 256, 128], P(None, 'row', 'col'), may hold values 0 or 1
- deriv_matrix: bfloat16 [2048, 2048], replicated, may hold values from -0.125 to 0.125
Outputs:
- filtered: bfloat16 [128, 2048, 2048], P('col', 'row')
- deriv_z: bfloat16 [128, 2048, 2048], P('col', 'row')
The draws below stay inside these ranges and needn't reach their ends.
Inputs may be any that keep to these rules, and one draw needn't show every extreme that they name: `solid_flags`: 1 marks a solid block, 0 a fluid one.
All inputs are finite; a program needn't handle non-finite values.
Results may differ from the reference program's by a relative error of at most 0.0058.
Values may be sent and summed in bfloat16 or wider, within the bound.
No kernel may reach another device: no remote copies, remote signals or barrier semaphores. Data moves between devices by JAX's collectives and lax.ppermute only.
A program may use at most 64 MiB of HBM per device.

```python
import jax
import jax.numpy as jnp
from jax import lax

NZ = 2048
YBLK = 8
ZBLK = 16
NX = 128
NY = 2048


def plant(drawn, rng, least, high):
    spot = [jax.random.randint(jax.random.fold_in(rng, axis), (), 0, length) for axis, length in enumerate(drawn.shape)]
    longest = drawn.shape.index(max(drawn.shape))
    neighbour = spot[:longest] + [(spot[longest] + 1) % drawn.shape[longest]] + spot[longest + 1:]
    return drawn.at[tuple(spot)].set(least).at[tuple(neighbour)].set(high)


def level_of(stream_key, shape, split, smallest, top_value):
    gain = 1.0
    for axis_at, blocks in split:
        steps = jax.random.uniform(jax.random.fold_in(jax.random.fold_in(stream_key, 6), axis_at), (blocks,), jnp.float32, smallest / len(split), top_value / len(split))
        gain = gain * jnp.repeat(jnp.exp(steps), shape[axis_at] // blocks).reshape((-1,) + (1,) * (len(shape) - 1 - axis_at))
    return gain


def gaussian(stream_key, extent, scale, most, split=(), kind=jnp.bfloat16):
    values = jax.random.normal(stream_key, extent, jnp.float32) * scale
    if len(split) > 0:
        values = level_of(stream_key, extent, split, -0.22, 0.18) * values
    return jnp.clip(values, min=-most, max=most).astype(kind)


def setup_inputs(seed: int = 0) -> dict:
    keys = jax.random.split(jax.random.key(seed), 4)
    field = gaussian(keys[0], (NX, NY, NZ), 1.0, 6.0, ((1, 16), (2, 16)))
    solid_flags = plant((jax.random.randint(keys[1], (NX, NY // YBLK, NZ // ZBLK), 0, 4) < 1).astype(jnp.int32), jax.random.fold_in(keys[1], 1), 0, 1)
    deriv_matrix = gaussian(keys[2], (NZ, NZ), NZ ** -0.5, 0.125)
    return {"field": field, "solid_flags": solid_flags, "deriv_matrix": deriv_matrix}


filter_taps = ((-3, 1.0), (-2, -6.0), (-1, 15.0), (0, -20.0), (1, 15.0), (2, -6.0), (3, 1.0))


def smooth(values, axis):
    total = values
    for offset, tap in filter_taps:
        total = total + (tap / 64.0) * jnp.roll(values, -offset, axis)
    return total


def reference(field, solid_flags, deriv_matrix):
    def one_plane(inputs):
        plane, flags = inputs
        blocks = flags.astype(jnp.float32)
        nyb, nzb = blocks.shape
        solid = jnp.broadcast_to(blocks[:, None, :, None], (nyb, YBLK, nzb, ZBLK)).reshape(nyb * YBLK, nzb * ZBLK)
        masked = plane.astype(jnp.float32) * (1.0 - solid)
        yfilt = smooth(masked, 0).astype(jnp.bfloat16)
        filtered = smooth(yfilt.astype(jnp.float32), 1).astype(jnp.bfloat16)
        deriv = jnp.dot(filtered, deriv_matrix, preferred_element_type=jnp.float32).astype(jnp.bfloat16)
        return filtered, deriv

    filtered, deriv_z = lax.map(one_plane, (field, solid_flags))
    return filtered, deriv_z
```

```python
import jax
import jax.numpy as jnp
import numpy as np
from jax import lax
from jax.experimental import pallas as pl
from jax.experimental.pallas import tpu as pltpu
from jax.sharding import PartitionSpec as P

YBLK = 8
ZBLK = 16
TAPS = {-3: 1.0, -2: -6.0, -1: 15.0, 0: 44.0, 1: 15.0, 2: -6.0, 3: 1.0}

EDGE = 16
HALO = 4
GROUP = 8


def tap_matrix(out_pos, in_pos):
    mat = np.zeros((len(out_pos), len(in_pos)), np.float32)
    for a, p in enumerate(out_pos):
        for b, q in enumerate(in_pos):
            if q is not None:
                mat[a, b] = TAPS.get(q - p, 0.0) / 64.0
    return mat


def keep_rows(flags_ref, keep_ref, planes):
    nyb, nzb = flags_ref.shape[1:]
    lane = lax.broadcasted_iota(jnp.int32, (nzb, nzb * ZBLK), 1) // ZBLK
    row = lax.broadcasted_iota(jnp.int32, (nzb, nzb * ZBLK), 0)
    spread = (lane == row).astype(jnp.float32)
    keep = (1 - flags_ref[...]).astype(jnp.float32).reshape(planes * nyb, nzb)
    wide = jnp.dot(keep, spread, preferred_element_type=jnp.float32)
    keep_ref[...] = wide.reshape(planes, nyb, nzb * ZBLK)


def masked_rows(field_ref, keep_ref, x, lo, hi):
    parts = []
    for b in range(lo // YBLK, hi // YBLK):
        parts.append(jnp.broadcast_to(keep_ref[x, pl.ds(b, 1), :], (YBLK, keep_ref.shape[2])))
    keep = jnp.concatenate(parts, axis=0)
    return field_ref[x, pl.ds(lo, hi - lo), :].astype(jnp.float32) * keep


def inner_body(field_ref, flags_ref, taps_ref, out_ref, low_ref, high_ref, keep_ref):
    planes, ycount, zcount = field_ref.shape
    keep_rows(flags_ref, keep_ref, planes)
    taps = taps_ref[...]
    for x in range(0, planes, 2):
        pair = []
        for k in range(2):
            m = masked_rows(field_ref, keep_ref, x + k, 0, ycount)
            high_ref[x + k] = m[:HALO].astype(jnp.bfloat16)
            low_ref[x + k] = m[ycount - HALO :].astype(jnp.bfloat16)
            pair.append(m.astype(jnp.bfloat16))
        res = jnp.dot(taps, jnp.concatenate(pair, axis=1), preferred_element_type=jnp.float32)
        for k in range(2):
            out_ref[x + k] = res[:, k * zcount : (k + 1) * zcount].astype(jnp.bfloat16)


def edge_body(field_ref, flags_ref, taps_ref, low_ref, high_ref, out_ref, keep_ref):
    planes, ycount, zcount = field_ref.shape
    keep_rows(flags_ref, keep_ref, planes)
    taps = taps_ref[...]
    for x in range(0, planes, 2):
        pair = []
        for k in range(2):
            top = masked_rows(field_ref, keep_ref, x + k, 0, 2 * EDGE)
            bottom = masked_rows(field_ref, keep_ref, x + k, ycount - 2 * EDGE, ycount)
            halo = jnp.concatenate(
                [low_ref[x + k].astype(jnp.float32), high_ref[x + k].astype(jnp.float32)], axis=0
            )
            halo = jnp.concatenate([halo, jnp.zeros_like(halo)], axis=0)
            pair.append(jnp.concatenate([top, bottom, halo], axis=0).astype(jnp.bfloat16))
        res = jnp.dot(taps, jnp.concatenate(pair, axis=1), preferred_element_type=jnp.float32)
        for k in range(2):
            out_ref[x + k] = res[:, k * zcount : (k + 1) * zcount].astype(jnp.bfloat16)


def inner_filter(field, flags):
    xcount, ycount, zcount = field.shape
    rows = ycount - 2 * EDGE
    taps = jnp.asarray(tap_matrix(range(EDGE, ycount - EDGE), range(ycount)), jnp.bfloat16)
    return pl.pallas_call(
        inner_body,
        grid=(xcount // GROUP,),
        in_specs=[
            pl.BlockSpec((GROUP, ycount, zcount), lambda i: (i, 0, 0)),
            pl.BlockSpec((GROUP,) + flags.shape[1:], lambda i: (i, 0, 0)),
            pl.BlockSpec(taps.shape, lambda i: (0, 0)),
        ],
        out_specs=[
            pl.BlockSpec((GROUP, rows, zcount), lambda i: (i, 0, 0)),
            pl.BlockSpec((GROUP, HALO, zcount), lambda i: (i, 0, 0)),
            pl.BlockSpec((GROUP, HALO, zcount), lambda i: (i, 0, 0)),
        ],
        out_shape=[
            jax.ShapeDtypeStruct((xcount, rows, zcount), jnp.bfloat16),
            jax.ShapeDtypeStruct((xcount, HALO, zcount), jnp.bfloat16),
            jax.ShapeDtypeStruct((xcount, HALO, zcount), jnp.bfloat16),
        ],
        scratch_shapes=[pltpu.VMEM((GROUP, ycount // YBLK, zcount), jnp.float32)],
        compiler_params=pltpu.CompilerParams(vmem_limit_bytes=8 << 20),
        name="inner_filter",
    )(field, flags, taps)


def edge_filter(field, flags, low, high):
    xcount, ycount, zcount = field.shape
    rows = 2 * EDGE
    top = list(range(2 * EDGE))
    bottom = list(range(ycount - 2 * EDGE, ycount))
    halo = list(range(-HALO, 0)) + list(range(ycount, ycount + HALO)) + [None] * (2 * HALO)
    outs = list(range(EDGE)) + list(range(ycount - EDGE, ycount))
    taps = jnp.asarray(tap_matrix(outs, top + bottom + halo), jnp.bfloat16)
    return pl.pallas_call(
        edge_body,
        grid=(xcount // GROUP,),
        in_specs=[
            pl.BlockSpec((GROUP, ycount, zcount), lambda i: (i, 0, 0)),
            pl.BlockSpec((GROUP,) + flags.shape[1:], lambda i: (i, 0, 0)),
            pl.BlockSpec(taps.shape, lambda i: (0, 0)),
            pl.BlockSpec((GROUP, HALO, zcount), lambda i: (i, 0, 0)),
            pl.BlockSpec((GROUP, HALO, zcount), lambda i: (i, 0, 0)),
        ],
        out_specs=pl.BlockSpec((GROUP, rows, zcount), lambda i: (i, 0, 0)),
        out_shape=jax.ShapeDtypeStruct((xcount, rows, zcount), jnp.bfloat16),
        scratch_shapes=[pltpu.VMEM((GROUP, ycount // YBLK, zcount), jnp.float32)],
        compiler_params=pltpu.CompilerParams(vmem_limit_bytes=8 << 20),
        name="edge_filter",
    )(field, flags, taps, low, high)


NBLK = 256


def finish_body(segments, first, *refs):
    slabs_ref, band_ref, deriv_ref = refs[:3]
    filt_out, deriv_out, filt, acc, fsem, dsem = refs[3 if first else 5 :]
    n = pl.program_id(0)
    steps = pl.num_programs(0)
    nslab, planes, rows, zb = slabs_ref.shape

    def filt_copies():
        return [
            pltpu.make_async_copy(
                filt.at[:, pl.ds(src, size), :], filt_out.at[:, pl.ds(dst, size), :], fsem.at[k]
            )
            for k, (src, dst, size) in enumerate(segments)
        ]

    def deriv_copies(step, slot):
        col = pl.multiple_of(step * NBLK, NBLK)
        return [
            pltpu.make_async_copy(
                acc.at[slot, :, pl.ds(src, size), :],
                deriv_out.at[:, pl.ds(dst, size), pl.ds(col, NBLK)],
                dsem.at[slot, k],
            )
            for k, (src, dst, size) in enumerate(segments)
        ]

    @pl.when(n == 0)
    def _():
        band = band_ref[...]
        for j in range(0, nslab, 2):
            window = [
                slabs_ref[(j + d) % nslab].reshape(planes * rows, zb) for d in (-1, 0, 1, 2)
            ]
            res = jnp.dot(
                jnp.concatenate(window, axis=1), band, preferred_element_type=jnp.float32
            )
            filt[:, :, pl.ds(j * zb, 2 * zb)] = res.astype(jnp.bfloat16).reshape(
                planes, rows, 2 * zb
            )
        for copy in filt_copies():
            copy.start()

    slot = n % 2

    @pl.when(n >= 2)
    def _():
        for copy in deriv_copies(n - 2, slot):
            copy.wait()

    flat = filt[...].reshape(planes * rows, nslab * zb)
    res = jnp.dot(flat, deriv_ref[...], preferred_element_type=jnp.float32)
    acc[slot] = res.astype(jnp.bfloat16).reshape(planes, rows, NBLK)
    for copy in deriv_copies(n, slot):
        copy.start()

    @pl.when(n == steps - 1)
    def _():
        for copy in filt_copies():
            copy.wait()
        for copy in deriv_copies(n - 1, 1 - slot):
            copy.wait()
        for copy in deriv_copies(n, slot):
            copy.wait()


def finish(slabs, deriv_matrix, segments, out_shape, partial=None):
    nslab, planes, rows, zb = slabs.shape
    zfull = nslab * zb
    band = jnp.asarray(tap_matrix(range(zb, 3 * zb), range(4 * zb)).T, jnp.bfloat16)
    nseg = len(segments)
    hbm = pl.BlockSpec(memory_space=pl.ANY)
    extra = () if partial is None else partial

    def body(*refs):
        finish_body(segments, partial is None, *refs)

    return pl.pallas_call(
        body,
        grid=(zfull // NBLK,),
        in_specs=[
            pl.BlockSpec(slabs.shape, lambda n: (0, 0, 0, 0)),
            pl.BlockSpec(band.shape, lambda n: (0, 0)),
            pl.BlockSpec((zfull, NBLK), lambda n: (0, n)),
        ]
        + [hbm] * len(extra),
        out_specs=[hbm, hbm],
        out_shape=[jax.ShapeDtypeStruct(out_shape, jnp.bfloat16)] * 2,
        input_output_aliases={} if partial is None else {3: 0, 4: 1},
        scratch_shapes=[
            pltpu.VMEM((planes, rows, zfull), jnp.bfloat16),
            pltpu.VMEM((2, planes, rows, NBLK), jnp.bfloat16),
            pltpu.SemaphoreType.DMA((nseg,)),
            pltpu.SemaphoreType.DMA((2, nseg)),
        ],
        compiler_params=pltpu.CompilerParams(
            dimension_semantics=("arbitrary",), vmem_limit_bytes=32 << 20
        ),
        name="finish_first" if partial is None else "finish_rest",
    )(slabs, band, deriv_matrix, *extra)


def shards(field, solid_flags, deriv_matrix):
    xcount, ycount, zcount = field.shape
    cols = lax.axis_size("col")
    count = lax.axis_size("row")
    inner, low, high = inner_filter(field, solid_flags)
    forward = [(i, (i + 1) % count) for i in range(count)]
    backward = [(target, source) for source, target in forward]
    from_low = lax.ppermute(low, "row", forward)
    from_high = lax.ppermute(high, "row", backward)
    inner_lines = lax.all_to_all(inner, "col", split_axis=0, concat_axis=0, tiled=True)
    edge = edge_filter(field, solid_flags, from_low, from_high)
    edge_lines = lax.all_to_all(edge, "col", split_axis=0, concat_axis=0, tiled=True)
    planes = xcount // cols
    out_shape = (planes, ycount, zcount * cols)
    part = finish(
        inner_lines.reshape(cols, planes, ycount - 2 * EDGE, zcount),
        deriv_matrix,
        ((0, EDGE, ycount - 2 * EDGE),),
        out_shape,
    )
    return tuple(
        finish(
            edge_lines.reshape(cols, planes, 2 * EDGE, zcount),
            deriv_matrix,
            ((0, 0, EDGE), (EDGE, ycount - EDGE, EDGE)),
            out_shape,
            part,
        )
    )


def solution(mesh):
    in_specs = (P(None, "row", "col"), P(None, "row", "col"), P())
    out_specs = (P("col", "row", None), P("col", "row", None))
    return jax.shard_map(shards, mesh=mesh, in_specs=in_specs, out_specs=out_specs, check_vma=False)
```

```python
import jax
import jax.numpy as jnp
import numpy as np
from jax import lax
from jax.experimental import pallas as pl
from jax.experimental.pallas import tpu as pltpu
from jax.sharding import PartitionSpec as P


YBLK = 8
ZBLK = 16
TAPS = {-3: 1.0, -2: -6.0, -1: 15.0, 0: 44.0, 1: 15.0, 2: -6.0, 3: 1.0}

EDGE = 16
HALO = 4
GROUP = 8
FIRST = 4
TILE = 16
ORDER = (
    (1, 0, 0), (0, 1, 0), (1, 1, 0), (0, 3, 0), (1, 3, 0),
    (0, 2, 0), (1, 2, 0), (0, 1, 1), (1, 0, 1), (0, 3, 1),
    (1, 1, 1), (0, 2, 1), (1, 3, 1), (1, 2, 1), (0, 0, 1),
)
OWN = (0, 0, 0)
BIG = 60 << 20


def tap_matrix(out_pos, in_pos):
    mat = np.zeros((len(out_pos), len(in_pos)), np.float32)
    for a, p in enumerate(out_pos):
        for b, q in enumerate(in_pos):
            if q is not None:
                mat[a, b] = TAPS.get(q - p, 0.0) / 64.0
    return mat


def shifted(index, offset, sign):
    x, y, c = index // 8, (index // 2) % 4, index % 2
    dx, dy, dc = offset
    return ((x + dx) % 2) * 8 + ((y + sign * dy + 4) % 4) * 2 + (c + dc) % 2


def expand_flags(flags_ref, keep_ref):
    nyb, nzb, _ = flags_ref.shape
    lane = lax.broadcasted_iota(jnp.int32, (nzb, nzb * ZBLK), 1) // ZBLK
    row = lax.broadcasted_iota(jnp.int32, (nzb, nzb * ZBLK), 0)
    spread = (lane == row).astype(jnp.float32)
    for b in range(nyb):
        keep = (1 - flags_ref[b]).astype(jnp.float32)
        keep_ref[b] = lax.dot_general(
            keep, spread, (((0,), (0,)), ((), ())), preferred_element_type=jnp.float32
        )


def masked_tile(rows, keep_ref, x, t):
    zcount = keep_ref.shape[2]
    keep = jnp.concatenate(
        [
            jnp.broadcast_to(keep_ref[b, pl.ds(x, 1), :], (YBLK, zcount))
            for b in range(t * TILE // YBLK, (t + 1) * TILE // YBLK)
        ],
        axis=0,
    )
    return rows * keep.astype(jnp.bfloat16)


def group_copies(field_ref, fbuf, sem, offsets, me):
    copies = []
    for k, offset in enumerate(offsets):
        start = pl.multiple_of(shifted(me, offset, 1) * GROUP, GROUP)
        copies.append(pltpu.make_async_copy(field_ref.at[pl.ds(start, GROUP)], fbuf.at[k], sem.at[k]))
    return copies


def filter_group(fbuf, k, base, keep_ref, taps, out_ref):
    _, planes, ycount, zcount = fbuf.shape
    for p in range(0, planes, 2):
        pair = []
        for q in (p, p + 1):
            tiles = [
                masked_tile(fbuf[k, q, pl.ds(t * TILE, TILE), :], keep_ref, base + q, t)
                for t in range(ycount // TILE)
            ]
            pair.append(jnp.concatenate(tiles, axis=0))
        res = jnp.dot(taps, jnp.concatenate(pair, axis=1), preferred_element_type=jnp.float32)
        out_ref[p] = res[:, :zcount].astype(jnp.bfloat16)
        out_ref[p + 1] = res[:, zcount:].astype(jnp.bfloat16)


def first_body(field_ref, flags_ref, taps_ref, *refs):
    outs, (keep_ref, fbuf, sem) = refs[:FIRST], refs[FIRST:]
    me = lax.axis_index("col")
    copies = group_copies(field_ref, fbuf, sem, ORDER[:FIRST], me)
    for copy in copies:
        copy.start()
    expand_flags(flags_ref, keep_ref)
    taps = taps_ref[...]
    for k, offset in enumerate(ORDER[:FIRST]):
        copies[k].wait()
        filter_group(fbuf, k, shifted(me, offset, 1) * GROUP, keep_ref, taps, outs[k])


def rest_body(field_ref, keep_ref, taps_ref, *refs):
    offsets = ORDER[FIRST:] + (OWN,) + ORDER[:FIRST]
    nout = len(ORDER) + 1 - FIRST
    outs, (low_ref, high_ref, fbuf, sem) = refs[:nout], refs[nout:]
    ycount, _ = fbuf.shape[2:]
    me = lax.axis_index("col")
    copies = group_copies(field_ref, fbuf, sem, offsets, me)
    for copy in copies:
        copy.start()
    taps = taps_ref[...]
    for k, offset in enumerate(offsets):
        copies[k].wait()
        base = shifted(me, offset, 1) * GROUP
        if k < nout:
            filter_group(fbuf, k, base, keep_ref, taps, outs[k])
        last = ycount // TILE - 1
        for q in range(GROUP):
            top = masked_tile(fbuf[k, q, pl.ds(0, TILE), :], keep_ref, base + q, 0)
            end = masked_tile(fbuf[k, q, pl.ds(last * TILE, TILE), :], keep_ref, base + q, last)
            high_ref[base + q] = top[:HALO]
            low_ref[base + q] = end[TILE - HALO :]


def inner_filter(field, flags):
    xcount, ycount, zcount = field.shape
    rows = ycount - 2 * EDGE
    taps = jnp.asarray(tap_matrix(range(EDGE, ycount - EDGE), range(ycount)), jnp.bfloat16)
    message = jax.ShapeDtypeStruct((GROUP, rows, zcount), jnp.bfloat16)
    halo = jax.ShapeDtypeStruct((xcount, HALO, zcount), jnp.bfloat16)
    keep = jax.ShapeDtypeStruct((ycount // YBLK, xcount, zcount), jnp.float32)
    hbm = pl.BlockSpec(memory_space=pl.ANY)
    vmem = pl.BlockSpec(memory_space=pltpu.VMEM)
    params = pltpu.CompilerParams(vmem_limit_bytes=24 << 20)

    def scratch(count):
        return [
            pltpu.VMEM((count, GROUP, ycount, zcount), jnp.bfloat16),
            pltpu.SemaphoreType.DMA((count,)),
        ]

    *sent, keep = pl.pallas_call(
        first_body,
        in_specs=[hbm, vmem, vmem],
        out_specs=[vmem] * (FIRST + 1),
        out_shape=[message] * FIRST + [keep],
        scratch_shapes=scratch(FIRST),
        compiler_params=params,
        name="first_messages",
    )(field, flags, taps)
    nout = len(ORDER) + 1 - FIRST
    *others, low, high = pl.pallas_call(
        rest_body,
        in_specs=[hbm, vmem, vmem],
        out_specs=[vmem] * (nout + 2),
        out_shape=[message] * nout + [halo, halo],
        scratch_shapes=scratch(len(ORDER) + 1),
        compiler_params=params,
        name="rest_messages",
    )(field, keep, taps)
    return sent + others, low, high, keep


def edge_body(field_ref, keep_ref, taps_ref, low_ref, high_ref, out_ref):
    planes, ycount, zcount = field_ref.shape
    taps = taps_ref[...]
    need = 2 * EDGE
    ntile = ycount // TILE
    picks = list(range(need // TILE)) + list(range(ntile - need // TILE, ntile))
    for x in range(0, planes, 2):
        pair = []
        for k in (x, x + 1):
            tiles = [masked_tile(field_ref[k, pl.ds(t * TILE, TILE), :], keep_ref, k, t) for t in picks]
            halo = jnp.concatenate(
                [low_ref[k].astype(jnp.float32), high_ref[k].astype(jnp.float32)], axis=0
            )
            halo = jnp.concatenate([halo, jnp.zeros_like(halo)], axis=0)
            pair.append(jnp.concatenate(tiles + [halo.astype(jnp.bfloat16)], axis=0))
        res = jnp.dot(taps, jnp.concatenate(pair, axis=1), preferred_element_type=jnp.float32)
        out_ref[x] = res[:, :zcount].astype(jnp.bfloat16)
        out_ref[x + 1] = res[:, zcount:].astype(jnp.bfloat16)


def edge_filter(field, keep, low, high):
    xcount, ycount, zcount = field.shape
    rows = 2 * EDGE
    top = list(range(2 * EDGE))
    bottom = list(range(ycount - 2 * EDGE, ycount))
    halo = list(range(-HALO, 0)) + list(range(ycount, ycount + HALO)) + [None] * (2 * HALO)
    outs = list(range(EDGE)) + list(range(ycount - EDGE, ycount))
    taps = jnp.asarray(tap_matrix(outs, top + bottom + halo), jnp.bfloat16)
    size = 2 * GROUP
    return pl.pallas_call(
        edge_body,
        grid=(xcount // size,),
        in_specs=[
            pl.BlockSpec((size, ycount, zcount), lambda i: (i, 0, 0)),
            pl.BlockSpec((keep.shape[0], size, zcount), lambda i: (0, i, 0)),
            pl.BlockSpec(taps.shape, lambda i: (0, 0)),
            pl.BlockSpec((size, HALO, zcount), lambda i: (i, 0, 0)),
            pl.BlockSpec((size, HALO, zcount), lambda i: (i, 0, 0)),
        ],
        out_specs=pl.BlockSpec((size, rows, zcount), lambda i: (i, 0, 0)),
        out_shape=jax.ShapeDtypeStruct((xcount, rows, zcount), jnp.bfloat16),
        compiler_params=pltpu.CompilerParams(vmem_limit_bytes=16 << 20),
        name="edge_filter",
    )(field, keep, taps, low, high)


NBLK = 256


def finish_body(segments, nin, nskip, *refs):
    lines, (band_ref, deriv_ref) = refs[:nin], refs[nin : nin + 2]
    filt_out, deriv_out, slabs_ref, filt, acc, ssem, fsem, dsem = refs[nin + 2 + nskip :]
    n = pl.program_id(0)
    steps = pl.num_programs(0)
    nslab, planes, rows, zb = slabs_ref.shape

    def slab_copies():
        if nin == 1:
            return [pltpu.make_async_copy(lines[0], slabs_ref, ssem.at[0])]
        me = lax.axis_index("col")
        return [
            pltpu.make_async_copy(line, slabs_ref.at[shifted(me, offset, -1)], ssem.at[k])
            for k, (line, offset) in enumerate(zip(lines, ORDER + (OWN,)))
        ]

    def filt_copies():
        return [
            pltpu.make_async_copy(
                filt.at[:, pl.ds(src, size), :], filt_out.at[:, pl.ds(dst, size), :], fsem.at[k]
            )
            for k, (src, dst, size) in enumerate(segments)
        ]

    def deriv_copies(step, slot):
        col = pl.multiple_of(step * NBLK, NBLK)
        return [
            pltpu.make_async_copy(
                acc.at[slot, :, pl.ds(src, size), :],
                deriv_out.at[:, pl.ds(dst, size), pl.ds(col, NBLK)],
                dsem.at[slot, k],
            )
            for k, (src, dst, size) in enumerate(segments)
        ]

    @pl.when(n == 0)
    def _():
        copies = slab_copies()
        for copy in copies:
            copy.start()
        for copy in copies:
            copy.wait()
        band = band_ref[...]
        for j in range(0, nslab, 2):
            window = [
                slabs_ref[(j + d) % nslab].reshape(planes * rows, zb) for d in (-1, 0, 1, 2)
            ]
            res = jnp.dot(
                jnp.concatenate(window, axis=1), band, preferred_element_type=jnp.float32
            )
            filt[:, :, pl.ds(j * zb, 2 * zb)] = res.astype(jnp.bfloat16).reshape(
                planes, rows, 2 * zb
            )
        for copy in filt_copies():
            copy.start()

    slot = n % 2

    @pl.when(n >= 2)
    def _():
        for copy in deriv_copies(n - 2, slot):
            copy.wait()

    flat = filt[...].reshape(planes * rows, nslab * zb)
    res = jnp.dot(flat, deriv_ref[...], preferred_element_type=jnp.float32)
    acc[slot] = res.astype(jnp.bfloat16).reshape(planes, rows, NBLK)
    for copy in deriv_copies(n, slot):
        copy.start()

    @pl.when(n == steps - 1)
    def _():
        for copy in filt_copies():
            copy.wait()
        for copy in deriv_copies(n - 1, 1 - slot):
            copy.wait()
        for copy in deriv_copies(n, slot):
            copy.wait()


def finish(lines, deriv_matrix, slab_shape, segments, out_shape, partial=()):
    nslab, planes, rows, zb = slab_shape
    zfull = nslab * zb
    band = jnp.asarray(tap_matrix(range(zb, 3 * zb), range(4 * zb)).T, jnp.bfloat16)
    nseg = len(segments)
    nin = len(lines)
    hbm = pl.BlockSpec(memory_space=pl.ANY)

    def body(*refs):
        finish_body(segments, nin, len(partial), *refs)

    return pl.pallas_call(
        body,
        grid=(zfull // NBLK,),
        in_specs=[hbm] * nin
        + [
            pl.BlockSpec(band.shape, lambda n: (0, 0)),
            pl.BlockSpec((zfull, NBLK), lambda n: (0, n)),
        ]
        + [hbm] * len(partial),
        out_specs=[hbm, hbm],
        out_shape=[jax.ShapeDtypeStruct(out_shape, jnp.bfloat16)] * 2,
        input_output_aliases={nin + 2 + k: k for k in range(len(partial))},
        scratch_shapes=[
            pltpu.VMEM(slab_shape, jnp.bfloat16),
            pltpu.VMEM((planes, rows, zfull), jnp.bfloat16),
            pltpu.VMEM((2, planes, rows, NBLK), jnp.bfloat16),
            pltpu.SemaphoreType.DMA((nin,)),
            pltpu.SemaphoreType.DMA((nseg,)),
            pltpu.SemaphoreType.DMA((2, nseg)),
        ],
        compiler_params=pltpu.CompilerParams(
            dimension_semantics=("arbitrary",), vmem_limit_bytes=BIG
        ),
        name="finish_rest" if partial else "finish_first",
    )(*lines, band, deriv_matrix, *partial)


def shards(field, solid_flags, deriv_matrix):
    xcount, ycount, zcount = field.shape
    cols = lax.axis_size("col")
    count = lax.axis_size("row")
    planes = xcount // cols
    out_shape = (planes, ycount, zcount * cols)
    messages, low, high, keep = inner_filter(field, solid_flags.transpose(1, 2, 0))
    lines = []
    for k, offset in enumerate(ORDER):
        pairs = [(i, shifted(i, offset, 1)) for i in range(cols)]
        lines.append(lax.ppermute(messages[k], "col", pairs))
    lines.append(messages[-1])
    forward = [(i, (i + 1) % count) for i in range(count)]
    backward = [(target, source) for source, target in forward]
    from_low = lax.ppermute(low, "row", forward)
    from_high = lax.ppermute(high, "row", backward)
    edge = edge_filter(field, keep, from_low, from_high)
    edge_lines = lax.all_to_all(edge, "col", split_axis=0, concat_axis=0, tiled=True)
    part = finish(
        lines,
        deriv_matrix,
        (cols, planes, ycount - 2 * EDGE, zcount),
        ((0, EDGE, ycount - 2 * EDGE),),
        out_shape,
    )
    slab_shape = (cols, planes, 2 * EDGE, zcount)
    return tuple(
        finish(
            [edge_lines.reshape(slab_shape)],
            deriv_matrix,
            slab_shape,
            ((0, 0, EDGE), (EDGE, ycount - EDGE, EDGE)),
            out_shape,
            tuple(part),
        )
    )


def solution(mesh):
    in_specs = (P(None, "row", "col"), P(None, "row", "col"), P())
    out_specs = (P("col", "row", None), P("col", "row", None))
    return jax.shard_map(shards, mesh=mesh, in_specs=in_specs, out_specs=out_specs, check_vma=False)
```
